32 devices in a mesh: grp: 4 (over z), seq: 8 (over y, x, core).
Axes of the slice: x: 2, y: 2, z: 4, core: 2. Of those that a mesh axis runs over, the one named last changes fastest.
Arguments:
- latent: bfloat16 [4, 256, 32, 256], P('grp', 'seq'), may hold values from -6 to 6
- up_key: bfloat16 [4, 128, 256], replicated, may hold values from -0.5 to 0.5
- up_value: bfloat16 [4, 128, 256], replicated, may hold values from -0.5 to 0.5
- queries: bfloat16 [8, 64, 128], replicated, may hold values from -240 to 240, as said below
- lengths: int32 [8], replicated, may hold values from 1 to 1024
- block_dest: int32 [256], replicated, may hold values from 0 to 31, as said below
Outputs:
- decode_latent: bfloat16 [32, 4, 8, 32, 256], P(('grp', 'seq'))
- attended: float32 [8, 8192], replicated
The draws below stay inside these ranges and needn't reach their ends.
Inputs may be any that keep to these rules, and one draw needn't show every extreme that they name: `block_dest`: each aligned run of 32 entries (the blocks of one seq index in the prefill layout) names every decode device exactly once. `queries`: the new token's query entries, real-valued.
All inputs are finite; a program needn't handle non-finite values.
Results may differ from the reference program's by a relative error of at most 0.001.
Values may be sent and summed in bfloat16 or wider, within the bound.
No kernel may reach another device: no remote copies, remote signals or barrier semaphores. Data moves between devices by JAX's collectives and lax.ppermute only.
A program may use at most 64 MiB of HBM per device.

```python
import jax
import jax.numpy as jnp
from jax import lax

Q_HEADS = 64
KV_HEADS = 8
HEAD_DIM = 128
RANK = 128
BATCH = 8
BT = 32
GROUPS = 4
DESTS = 32
BLOCKS = 256
S_MAX = 1024


def draw_queries(key, part):
    drawn = jnp.clip(jax.random.normal(key, (BATCH, Q_HEADS, HEAD_DIM), jnp.float32), -4.0, 4.0)
    return drawn.astype(jnp.bfloat16)


def draw_block_dest(key, part):
    shards = BLOCKS // DESTS
    subkeys = jax.random.split(jax.random.fold_in(key, 11), shards)
    orders = jax.vmap(lambda subkey: jax.random.permutation(subkey, DESTS))(subkeys)
    return orders.reshape(BLOCKS).astype(jnp.int32)


def place_ends(values, key, least, largest):
    place = [jax.random.randint(jax.random.fold_in(key, axis), (), 0, length) for axis, length in enumerate(values.shape)]
    main_axis = values.shape.index(max(values.shape))
    next_to = place[:main_axis] + [(place[main_axis] + 1) % values.shape[main_axis]] + place[main_axis + 1:]
    return values.at[tuple(place)].set(least).at[tuple(next_to)].set(largest)


def steps_of(stream_key, shape, cuts, smallest, high):
    loudness = 1.0
    for position, blocks in cuts:
        steps = jax.random.uniform(jax.random.fold_in(jax.random.fold_in(stream_key, 6), position), (blocks,), jnp.float32, smallest / len(cuts), high / len(cuts))
        loudness = loudness * jnp.repeat(jnp.exp(steps), shape[position] // blocks).reshape((-1,) + (1,) * (len(shape) - 1 - position))
    return loudness


def noise(key, extent, spread, bound, pieces=(), kind=jnp.bfloat16):
    entries = spread * jax.random.normal(key, extent, jnp.float32)
    if pieces:
        entries = entries * steps_of(key, extent, pieces, -0.22, 0.18)
    return jnp.clip(entries, -bound, bound).astype(kind)


def setup_inputs(seed: int = 0) -> dict:
    streams_of = jax.random.split(jax.random.key(seed), 7)
    latent = noise(streams_of[0], (GROUPS, BLOCKS, BT, 2 * RANK), 1.0, 6.0, ((0, 4), (1, 8)))
    up_key = noise(streams_of[1], (GROUPS, RANK, KV_HEADS // GROUPS * HEAD_DIM), RANK ** -0.5, 0.5)
    up_value = noise(streams_of[2], (GROUPS, RANK, KV_HEADS // GROUPS * HEAD_DIM), RANK ** -0.5, 0.5)
    queries = draw_queries(jax.random.fold_in(streams_of[6], 71), 0)
    lengths = place_ends(jax.random.randint(streams_of[4], (BATCH,), 1, S_MAX + 1), jax.random.fold_in(streams_of[4], 1), 1, S_MAX).astype(jnp.int32)
    block_dest = draw_block_dest(jax.random.fold_in(streams_of[6], 71), 0)
    return dict(latent=latent, up_key=up_key, up_value=up_value, queries=queries, lengths=lengths, block_dest=block_dest)


def reference(latent, up_key, up_value, queries, lengths, block_dest):
    shards = BLOCKS // DESTS
    table = block_dest.reshape(shards, DESTS)
    row_ids = jnp.broadcast_to(jnp.arange(shards, dtype=jnp.int32)[:, None], (shards, DESTS))
    col_ids = jnp.broadcast_to(jnp.arange(DESTS, dtype=jnp.int32)[None, :], (shards, DESTS))
    source_order = jnp.zeros((shards, DESTS), jnp.int32).at[row_ids, table].set(col_ids)
    global_ids = row_ids * DESTS + source_order
    picked = latent[:, global_ids.T]
    decode_latent = jnp.transpose(picked, (1, 0, 2, 3, 4))
    per_group = KV_HEADS // GROUPS
    per_kv = Q_HEADS // KV_HEADS
    scale = 1.0 / math_sqrt(HEAD_DIM)
    query_f = queries.astype(jnp.float32).reshape(BATCH, GROUPS, per_group, per_kv, HEAD_DIM)
    positions = jnp.arange(S_MAX, dtype=jnp.int32)
    valid = positions[None, :] < lengths[:, None]

    def one_group(index):
        lat = lax.dynamic_index_in_dim(latent, index, 0, keepdims=False).astype(jnp.float32)
        lat = lat.reshape(BATCH, S_MAX, 2 * RANK)
        key_map = lax.dynamic_index_in_dim(up_key, index, 0, keepdims=False).astype(jnp.float32)
        value_map = lax.dynamic_index_in_dim(up_value, index, 0, keepdims=False).astype(jnp.float32)
        keys = jnp.einsum('bsr,rc->bsc', lat[..., :RANK], key_map, precision=lax.Precision.HIGHEST)
        values = jnp.einsum('bsr,rc->bsc', lat[..., RANK:], value_map, precision=lax.Precision.HIGHEST)
        keys = keys.reshape(BATCH, S_MAX, per_group, HEAD_DIM)
        values = values.reshape(BATCH, S_MAX, per_group, HEAD_DIM)
        query_g = lax.dynamic_index_in_dim(query_f, index, 1, keepdims=False)
        scores = jnp.einsum('bkjd,bskd->bkjs', query_g, keys, precision=lax.Precision.HIGHEST) * scale
        live = valid[:, None, None, :]
        scores = jnp.where(live, scores, -1e+30)
        row_max = lax.optimization_barrier(jnp.max(scores, axis=-1, keepdims=True))
        weights = jnp.where(live, jnp.exp(scores - row_max), 0.0)
        totals = lax.optimization_barrier(jnp.sum(weights, axis=-1))
        summed = jnp.einsum('bkjs,bskd->bkjd', weights, values, precision=lax.Precision.HIGHEST)
        return summed / totals[..., None]
    outputs = lax.map(one_group, jnp.arange(GROUPS, dtype=jnp.int32))
    attended = jnp.transpose(outputs, (1, 0, 2, 3, 4)).reshape(BATCH, Q_HEADS * HEAD_DIM)
    return (decode_latent, attended)

def math_sqrt(value):
    return float(value) ** 0.5
```

```python
import functools

import jax
import jax.numpy as jnp
from jax import lax
from jax.experimental import pallas as pl
from jax.experimental.pallas import tpu as pltpu
from jax.sharding import PartitionSpec as P


AXES = ("grp", "seq")
F32 = jnp.float32
BF16 = jnp.bfloat16


def three_parts(x):
    high = x.astype(BF16)
    rest = x - high.astype(F32)
    middle = rest.astype(BF16)
    low = (rest - middle.astype(F32)).astype(BF16)
    return jnp.concatenate([high, middle, low], axis=0)


def exact_dot(x, y, contract):
    rows = x.shape[0]
    wide = lax.dot_general(
        three_parts(x), y, ((contract), ((), ())), preferred_element_type=F32
    )
    return wide[:rows] + (wide[rows : 2 * rows] + wide[2 * rows :])


def relayout_kernel(dest_hbm, lat_hbm, out_ref, nat_ref, dest_smem, sems):
    slots = lat_hbm.shape[0]
    first = lax.axis_index("seq") * slots
    get_dest = pltpu.make_async_copy(dest_hbm, dest_smem, sems.at[0])
    get_lat = pltpu.make_async_copy(lat_hbm, nat_ref, sems.at[1])
    get_dest.start()
    get_lat.start()
    get_dest.wait()
    get_lat.wait()

    def move(j, carry):
        out_ref[dest_smem[first + j]] = nat_ref[j]
        return carry

    lax.fori_loop(0, slots, move, 0, unroll=8)


def relayout(block_dest, latent):
    return pl.pallas_call(
        relayout_kernel,
        out_shape=(
            jax.ShapeDtypeStruct(latent.shape, latent.dtype),
            jax.ShapeDtypeStruct(latent.shape, latent.dtype),
        ),
        in_specs=[pl.BlockSpec(memory_space=pl.ANY)] * 2,
        out_specs=(pl.BlockSpec(memory_space=pltpu.VMEM),) * 2,
        scratch_shapes=[
            pltpu.SMEM(block_dest.shape, jnp.int32),
            pltpu.SemaphoreType.DMA((2,)),
        ],
        name="relayout",
    )(block_dest, latent)


def attend_kernel(per_seq, block_len, lat_ref, key_ref, value_ref, query_ref, length_ref, *outs):
    slots = lat_ref.shape[0]
    rank = lat_ref.shape[2] // 2
    head_dim = query_ref.shape[2]
    per_group = key_ref.shape[2] // head_dim
    heads = query_ref.shape[1] // key_ref.shape[0]
    per_kv = heads // per_group
    scale = 1.0 / float(head_dim) ** 0.5
    group = lax.axis_index("grp")
    block = lax.axis_index("seq") * slots
    seq = block // per_seq
    start = (block % per_seq) * block_len
    length = length_ref[seq]
    tokens = slots * block_len
    lat = lat_ref[...].reshape(tokens, 2 * rank)
    query = query_ref[seq, pl.ds(pl.multiple_of(group * heads, heads), heads), :]
    absorbed = []
    for k in range(per_group):
        q = query[k * per_kv : (k + 1) * per_kv]
        u = key_ref[group, :, k * head_dim : (k + 1) * head_dim]
        absorbed.append(
            lax.dot_general(q, u, (((1,), (1,)), ((), ())), preferred_element_type=F32)
        )
    absorbed = jnp.concatenate(absorbed, axis=0)
    scores = exact_dot(absorbed, lat[:, :rank], ((1,), (1,))) * scale
    position = start + lax.broadcasted_iota(jnp.int32, scores.shape, 1)
    live = position < length
    scores = jnp.where(live, scores, -1e30)
    top = jnp.max(scores, axis=1, keepdims=True)
    weights = jnp.where(live, jnp.exp(scores - top), 0.0)
    total = jnp.sum(weights, axis=1, keepdims=True)
    mixed = exact_dot(weights, lat[:, rank:], ((1,), (0,)))
    attended = []
    for k in range(per_group):
        u = value_ref[group, :, k * head_dim : (k + 1) * head_dim]
        attended.append(exact_dot(mixed[k * per_kv : (k + 1) * per_kv], u, ((1,), (0,))))
    attended = jnp.concatenate(attended, axis=0)
    (out_ref,) = outs
    if out_ref.shape[1] == heads:
        rows = attended / total
    else:
        rows = jnp.concatenate(
            [attended, jnp.broadcast_to(top, attended.shape), jnp.broadcast_to(total, attended.shape)],
            axis=0,
        )
    for d in range(out_ref.shape[0]):
        out_ref[d] = rows


def attend(latent, up_key, up_value, queries, lengths, dests, spans, per_seq):
    heads = queries.shape[1] // up_key.shape[0]
    rows = heads if spans == 1 else 3 * heads
    vmem = pl.BlockSpec(memory_space=pltpu.VMEM)
    return pl.pallas_call(
        functools.partial(attend_kernel, per_seq, latent.shape[1]),
        out_shape=jax.ShapeDtypeStruct((dests, rows, queries.shape[2]), F32),
        in_specs=[vmem] * 4 + [pl.BlockSpec(memory_space=pltpu.SMEM)],
        out_specs=vmem,
        name="attend",
    )(latent, up_key, up_value, queries, lengths)


def gathered_by_pairs(x, axis):
    size = lax.axis_size(axis)
    step = 1
    while step < size:
        pairs = [[i, i + step] for i in range(size) if not i & step]
        x = lax.all_gather(x, axis, axis=0, tiled=True, axis_index_groups=pairs)
        step *= 2
    return x


def body(latent, up_key, up_value, queries, lengths, block_dest):
    groups = up_key.shape[0]
    slots = latent.shape[1]
    batch = queries.shape[0]
    heads = queries.shape[1] // groups
    head_dim = queries.shape[2]
    per_seq = block_dest.shape[0] // batch
    shards = lax.axis_size("seq")
    spans = per_seq // slots
    assert spans * slots == per_seq and spans * batch == shards

    outgoing, natural = relayout(block_dest, latent[0])
    received = lax.all_to_all(outgoing, AXES, split_axis=0, concat_axis=0, tiled=True)
    decode_latent = received.reshape((1, groups, shards) + latent.shape[2:])

    mine = attend(natural, up_key, up_value, queries, lengths, 1, spans, per_seq)
    mine = gathered_by_pairs(mine, "grp")
    every = lax.all_gather(mine, "seq", axis=0)
    every = jnp.swapaxes(every, 0, 1)
    every = every.reshape(groups, batch, spans, -1, head_dim)
    if spans == 1:
        result = every[:, :, 0]
    else:
        accum, top, total = (every[:, :, :, k * heads : (k + 1) * heads] for k in range(3))
        factor = jnp.exp(top - jnp.max(top, axis=2, keepdims=True))
        result = jnp.sum(accum * factor, axis=2) / jnp.sum(total * factor, axis=2)
    attended = jnp.transpose(result, (1, 0, 2, 3)).reshape(batch, groups * heads * head_dim)
    return (decode_latent, attended)


def solution(mesh):
    return jax.shard_map(
        body,
        mesh=mesh,
        in_specs=(P("grp", "seq", None, None), P(), P(), P(), P(), P()),
        out_specs=(P(AXES, None, None, None, None), P()),
        check_vma=False,
    )
```

```python
import functools
import math

import jax
import jax.numpy as jnp
from jax import lax
from jax.experimental import pallas as pl
from jax.experimental.pallas import tpu as pltpu
from jax.sharding import PartitionSpec as P

AXES = ("grp", "seq")
F32 = jnp.float32
BF16 = jnp.bfloat16
NEAR_BYTES = 1 << 20


def parts_of(x, count):
    parts = []
    for _ in range(count):
        part = x.astype(BF16)
        parts.append(part)
        x = x - part.astype(F32)
    return parts


def exact_dot(x, y, contract):
    rows = x.shape[0]
    wide = lax.dot_general(
        jnp.concatenate(parts_of(x, 3), axis=0),
        y,
        (contract, ((), ())),
        preferred_element_type=F32,
    )
    return wide[:rows] + (wide[rows : 2 * rows] + wide[2 * rows :])


def in_vmem(shape):
    return 2 * math.prod(shape) <= NEAR_BYTES


def start_kernel(
    per_seq,
    sent,
    dest_hbm,
    length_hbm,
    lat_hbm,
    key_hbm,
    value_hbm,
    query_hbm,
    out_ref,
    dest,
    length,
    lat_ref,
    key_ref,
    value_ref,
    query_ref,
    sems,
):
    slots, block_len, width = lat_ref.shape
    rank = width // 2
    heads, head_dim = query_ref.shape
    per_group = key_ref.shape[1] // head_dim
    per_kv = heads // per_group
    scale = 1.0 / float(head_dim) ** 0.5
    group = lax.axis_index("grp")
    first = lax.axis_index("seq") * slots
    seq = first // per_seq
    start = (first % per_seq) * block_len
    rows = pl.ds(pl.multiple_of(group * heads, heads), heads)
    sources = (lat_hbm, dest_hbm, key_hbm.at[group], query_hbm.at[seq, rows], length_hbm, value_hbm.at[group])
    targets = (lat_ref, dest, key_ref, query_ref, length, value_ref)
    copies = [
        pltpu.make_async_copy(source, target, sems.at[k])
        for k, (source, target) in enumerate(zip(sources, targets))
    ]
    for copy in copies:
        copy.start()
    for copy in copies:
        copy.wait()

    def move(j, carry):
        out_ref[dest[first + j], :block_len, :] = lat_ref[j]
        return carry

    lax.fori_loop(0, slots, move, 0, unroll=8)

    tokens = slots * block_len
    lat = lat_ref[...].reshape(tokens, width)
    absorbed = []
    for k in range(per_group):
        columns = slice(k * head_dim, (k + 1) * head_dim)
        absorbed.append(
            lax.dot_general(
                query_ref[k * per_kv : (k + 1) * per_kv, :],
                key_ref[:, columns],
                (((1,), (1,)), ((), ())),
                preferred_element_type=F32,
            )
        )
    absorbed = jnp.concatenate(absorbed, axis=0)
    scores = exact_dot(absorbed, lat[:, :rank], ((1,), (1,))) * scale
    position = start + lax.broadcasted_iota(jnp.int32, scores.shape, 1)
    live = position < length[seq]
    scores = jnp.where(live, scores, -1e30)
    top = jnp.max(scores, axis=1, keepdims=True)
    weights = jnp.where(live, jnp.exp(scores - top), 0.0)
    total = jnp.sum(weights, axis=1, keepdims=True)
    mixed = exact_dot(weights, lat[:, rank:], ((1,), (0,)))
    if per_seq == slots:
        mixed = mixed / total
    attended = []
    for k in range(per_group):
        columns = slice(k * head_dim, (k + 1) * head_dim)
        attended.append(
            exact_dot(mixed[k * per_kv : (k + 1) * per_kv], value_ref[:, columns], ((1,), (0,)))
        )
    fields = [jnp.concatenate(attended, axis=1)]
    if per_seq != slots:
        for field in (top, total):
            fields.append(
                jnp.concatenate(
                    [
                        jnp.broadcast_to(field[k * per_kv : (k + 1) * per_kv], (per_kv, head_dim))
                        for k in range(per_group)
                    ],
                    axis=1,
                )
            )
    extra = jnp.concatenate([part for field in fields for part in parts_of(field, sent)], axis=0)
    for d in range(out_ref.shape[0]):
        out_ref[d, block_len:, :] = extra


def start(latent, up_key, up_value, queries, lengths, block_dest, dests, extra_rows, sent):
    slots, block_len, width = latent.shape
    batch, q_heads, head_dim = queries.shape
    groups = up_key.shape[0]
    per_seq = block_dest.shape[0] // batch
    shape = (dests, block_len + extra_rows, width)
    near = in_vmem(shape)
    return pl.pallas_call(
        functools.partial(start_kernel, per_seq, sent),
        out_shape=(pltpu.VMEM if near else jax.ShapeDtypeStruct)(shape, latent.dtype),
        in_specs=[pl.BlockSpec(memory_space=pl.ANY)] * 6,
        out_specs=pl.BlockSpec(memory_space=pltpu.VMEM),
        scratch_shapes=[
            pltpu.SMEM(block_dest.shape, jnp.int32),
            pltpu.SMEM(lengths.shape, jnp.int32),
            pltpu.VMEM(latent.shape, latent.dtype),
            pltpu.VMEM(up_key.shape[1:], up_key.dtype),
            pltpu.VMEM(up_value.shape[1:], up_value.dtype),
            pltpu.VMEM((q_heads // groups, head_dim), queries.dtype),
            pltpu.SemaphoreType.DMA((6,)),
        ],
        name="start",
    )(block_dest, lengths, latent, up_key, up_value, queries)


def finish_kernel(spans, sent, head_dim, got_ref, decode_hbm, result_hbm, result_ref, wide_ref, sems):
    block_len = decode_hbm.shape[1]
    batch, columns = result_ref.shape
    copy_blocks = pltpu.make_async_copy(got_ref.at[:, :block_len, :], decode_hbm, sems.at[0])
    copy_blocks.start()
    width = got_ref.shape[2]
    per_group = width // head_dim
    fields = 1 if spans == 1 else 3
    per_kv = (got_ref.shape[1] - block_len) // (sent * fields)
    groups = got_ref.shape[0] // (batch * spans)

    def field(source, k):
        begin = block_len + k * sent * per_kv
        return sum(
            got_ref[source, begin + p * per_kv : begin + (p + 1) * per_kv, :].astype(F32)
            for p in reversed(range(sent))
        )

    for g in range(groups):
        for b in range(batch):
            sources = [(g * batch + b) * spans + k for k in range(spans)]
            if spans == 1:
                value = field(sources[0], 0)
            else:
                tops = [field(source, 1) for source in sources]
                top = functools.reduce(jnp.maximum, tops)
                factors = [jnp.exp(t - top) for t in tops]
                total = sum(field(source, 2) * f for source, f in zip(sources, factors))
                value = sum(field(source, 0) * f for source, f in zip(sources, factors)) / total
            wide_ref[g, b] = value
    for g in range(groups):
        for k in range(per_group):
            for j in range(per_kv):
                column = ((g * per_group + k) * per_kv + j) * head_dim
                result_ref[:, column : column + head_dim] = wide_ref[
                    g, :, j, k * head_dim : (k + 1) * head_dim
                ]
    copy_result = pltpu.make_async_copy(result_ref, result_hbm, sems.at[1])
    copy_result.start()
    copy_blocks.wait()
    copy_result.wait()


def finish(got, block_len, batch, columns, head_dim, spans, sent):
    dests, rows, width = got.shape
    groups = dests // (batch * spans)
    per_kv = columns // (groups * width)
    if in_vmem(got.shape):
        got = pltpu.with_memory_space_constraint(got, pltpu.VMEM)
    return pl.pallas_call(
        functools.partial(finish_kernel, spans, sent, head_dim),
        out_shape=(
            jax.ShapeDtypeStruct((dests, block_len, width), got.dtype),
            jax.ShapeDtypeStruct((batch, columns), F32),
        ),
        in_specs=[pl.BlockSpec(memory_space=pltpu.VMEM)],
        out_specs=(pl.BlockSpec(memory_space=pl.ANY),) * 2,
        scratch_shapes=[
            pltpu.VMEM((batch, columns), F32),
            pltpu.VMEM((groups, batch, per_kv, width), F32),
            pltpu.SemaphoreType.DMA((2,)),
        ],
        name="finish",
    )(got)


def body(latent, up_key, up_value, queries, lengths, block_dest):
    groups = up_key.shape[0]
    slots, block_len, width = latent.shape[1:]
    batch, q_heads, head_dim = queries.shape
    shards = lax.axis_size("seq")
    dests = groups * shards
    spans = shards // batch
    assert spans * batch == shards and up_key.shape[2] == width
    sent, fields = (2, 1) if spans == 1 else (3, 3)
    per_kv = q_heads * head_dim // (groups * width)
    payload = start(
        latent[0], up_key, up_value, queries, lengths, block_dest, dests, sent * fields * per_kv, sent
    )
    got = lax.all_to_all(payload, AXES, split_axis=0, concat_axis=0, tiled=True)
    decode, attended = finish(got, block_len, batch, q_heads * head_dim, head_dim, spans, sent)
    return (decode.reshape(1, groups, shards, block_len, width), attended)


def solution(mesh):
    return jax.shard_map(
        body,
        mesh=mesh,
        in_specs=(P("grp", "seq", None, None), P(), P(), P(), P(), P()),
        out_specs=(P(AXES, None, None, None, None), P()),
        check_vma=False,
    )
```

```python
import functools
import math

import jax
import jax.numpy as jnp
from jax import lax
from jax.experimental import pallas as pl
from jax.experimental.pallas import tpu as pltpu
from jax.sharding import PartitionSpec as P


AXES = ("grp", "seq")
F32 = jnp.float32
BF16 = jnp.bfloat16
NEAR_BYTES = 1 << 20
NEAR_DEVICES = 4


def three_parts(x):
    parts = []
    for _ in range(3):
        part = x.astype(BF16)
        parts.append(part)
        x = x - part.astype(F32)
    return jnp.concatenate(parts, axis=0)


def exact_dot(x, y, contract):
    rows = x.shape[0]
    wide = lax.dot_general(
        three_parts(x),
        y,
        (contract, ((), ())),
        preferred_element_type=F32,
    )
    return wide[:rows] + (wide[rows : 2 * rows] + wide[2 * rows :])


def in_vmem(shape):
    return 4 * math.prod(shape) <= NEAR_BYTES


def start_kernel(
    per_seq,
    dest_hbm,
    length_hbm,
    lat_hbm,
    key_hbm,
    value_hbm,
    query_hbm,
    out_hbm,
    mine_ref,
    dest,
    length,
    lat_ref,
    key_ref,
    value_ref,
    query_ref,
    ordered_ref,
    sems,
):
    slots, block_len, width = lat_ref.shape
    rank = width // 2
    heads, head_dim = query_ref.shape
    per_group = key_ref.shape[1] // head_dim
    per_kv = heads // per_group
    scale = 1.0 / float(head_dim) ** 0.5
    group = lax.axis_index("grp")
    first = lax.axis_index("seq") * slots
    seq = first // per_seq
    start = (first % per_seq) * block_len
    rows = pl.ds(pl.multiple_of(group * heads, heads), heads)
    sources = (lat_hbm, dest_hbm, key_hbm.at[group], query_hbm.at[seq, rows], length_hbm, value_hbm.at[group])
    targets = (lat_ref, dest, key_ref, query_ref, length, value_ref)
    copies = [
        pltpu.make_async_copy(source, target, sems.at[k])
        for k, (source, target) in enumerate(zip(sources, targets))
    ]
    for copy in copies:
        copy.start()
    for copy in copies:
        copy.wait()

    def move(j, carry):
        ordered_ref[dest[first + j]] = lat_ref[j]
        return carry

    lax.fori_loop(0, slots, move, 0, unroll=8)
    send = pltpu.make_async_copy(ordered_ref, out_hbm, sems.at[len(copies)])
    send.start()

    tokens = slots * block_len
    lat = lat_ref[...].reshape(tokens, width)
    absorbed = []
    for k in range(per_group):
        columns = slice(k * head_dim, (k + 1) * head_dim)
        absorbed.append(
            lax.dot_general(
                query_ref[k * per_kv : (k + 1) * per_kv, :],
                key_ref[:, columns],
                (((1,), (1,)), ((), ())),
                preferred_element_type=F32,
            )
        )
    absorbed = jnp.concatenate(absorbed, axis=0)
    scores = exact_dot(absorbed, lat[:, :rank], ((1,), (1,))) * scale
    position = start + lax.broadcasted_iota(jnp.int32, scores.shape, 1)
    live = position < length[seq]
    scores = jnp.where(live, scores, -1e30)
    top = jnp.max(scores, axis=1, keepdims=True)
    weights = jnp.where(live, jnp.exp(scores - top), 0.0)
    total = jnp.sum(weights, axis=1, keepdims=True)
    mixed = exact_dot(weights, lat[:, rank:], ((1,), (0,)))
    if per_seq == slots:
        mixed = mixed / total
    attended = []
    for k in range(per_group):
        columns = slice(k * head_dim, (k + 1) * head_dim)
        attended.append(
            exact_dot(mixed[k * per_kv : (k + 1) * per_kv], value_ref[:, columns], ((1,), (0,)))
        )
    fields = [jnp.concatenate(attended, axis=0)]
    if per_seq != slots:
        fields += [jnp.broadcast_to(field, (heads, head_dim)) for field in (top, total)]
    mine_ref[...] = jnp.concatenate(fields, axis=0)
    send.wait()


def start(latent, up_key, up_value, queries, lengths, block_dest):
    batch, q_heads, head_dim = queries.shape
    heads = q_heads // up_key.shape[0]
    per_seq = block_dest.shape[0] // batch
    rows = heads if per_seq == latent.shape[0] else 3 * heads
    return pl.pallas_call(
        functools.partial(start_kernel, per_seq),
        out_shape=(
            jax.ShapeDtypeStruct(latent.shape, latent.dtype),
            pltpu.VMEM((rows, head_dim), F32),
        ),
        in_specs=[pl.BlockSpec(memory_space=pl.ANY)] * 6,
        out_specs=(pl.BlockSpec(memory_space=pl.ANY), pl.BlockSpec(memory_space=pltpu.VMEM)),
        scratch_shapes=[
            pltpu.SMEM(block_dest.shape, jnp.int32),
            pltpu.SMEM(lengths.shape, jnp.int32),
            pltpu.VMEM(latent.shape, latent.dtype),
            pltpu.VMEM(up_key.shape[1:], up_key.dtype),
            pltpu.VMEM(up_value.shape[1:], up_value.dtype),
            pltpu.VMEM((heads, head_dim), queries.dtype),
            pltpu.VMEM(latent.shape, latent.dtype),
            pltpu.SemaphoreType.DMA((7,)),
        ],
        name="start",
    )(block_dest, lengths, latent, up_key, up_value, queries)


def finish_kernel(groups, shards, offsets, heads, *refs):
    sources, (result_hbm, result_ref, wide_ref, sem) = refs[: len(offsets)], refs[len(offsets) :]
    batch = result_ref.shape[0]
    spans = shards // batch
    near, halves, _, head_dim = sources[0].shape
    group = lax.axis_index("grp")
    major = lax.axis_index("seq") // near
    for (step, flip), source in zip(offsets, sources):
        from_major = (major + step) % (shards // near)
        for half in range(halves):
            from_group = group ^ flip ^ (half * (groups // 2))
            for k in range(near):
                wide_ref[from_group, from_major * near + k] = source[k, half]
    if spans > 1:
        for g in range(groups):
            for b in range(batch):
                parts = [wide_ref[g, b * spans + k] for k in range(spans)]
                accums, tops, totals = (
                    [part[f * heads : (f + 1) * heads] for part in parts] for f in range(3)
                )
                top = functools.reduce(jnp.maximum, tops)
                factors = [jnp.exp(t - top) for t in tops]
                accum = sum(x * f for x, f in zip(accums, factors))
                total = sum(x * f for x, f in zip(totals, factors))
                wide_ref[g, b, :heads] = accum / total
    for g in range(groups):
        for h in range(heads):
            column = (g * heads + h) * head_dim
            result_ref[:, column : column + head_dim] = wide_ref[g, :batch, h, :]
    copy = pltpu.make_async_copy(result_ref, result_hbm, sem)
    copy.start()
    copy.wait()


def finish(pieces, offsets, groups, shards, batch, heads):
    rows, head_dim = pieces[0].shape[2:]
    columns = groups * heads * head_dim
    if in_vmem((len(pieces),) + pieces[0].shape):
        pieces = [pltpu.with_memory_space_constraint(piece, pltpu.VMEM) for piece in pieces]
    return pl.pallas_call(
        functools.partial(finish_kernel, groups, shards, offsets, heads),
        out_shape=jax.ShapeDtypeStruct((batch, columns), F32),
        in_specs=[pl.BlockSpec(memory_space=pltpu.VMEM)] * len(pieces),
        out_specs=pl.BlockSpec(memory_space=pl.ANY),
        scratch_shapes=[
            pltpu.VMEM((batch, columns), F32),
            pltpu.VMEM((groups, shards, rows, head_dim), F32),
            pltpu.SemaphoreType.DMA,
        ],
        name="finish",
    )(*pieces)


def body(latent, up_key, up_value, queries, lengths, block_dest):
    groups = up_key.shape[0]
    _, block_len, width = latent.shape[1:]
    batch, q_heads, _ = queries.shape
    shards = lax.axis_size("seq")
    near = math.gcd(shards, NEAR_DEVICES)
    far = shards // near
    assert groups % 2 == 0 and shards % batch == 0
    payload, mine = start(latent[0], up_key, up_value, queries, lengths, block_dest)
    other = lax.ppermute(mine, "grp", [(i, i ^ (groups // 2)) for i in range(groups)])
    got = lax.all_to_all(payload, AXES, split_axis=0, concat_axis=0, tiled=True)
    both = jnp.stack([mine, other])
    neighbours = [[k * near + i for i in range(near)] for k in range(far)]
    plane = lax.all_gather(both, "seq", axis=0, axis_index_groups=neighbours)
    offsets = [(step, flip) for flip in range(groups // 2) for step in range(far)]
    pieces = [plane]
    for step, flip in offsets[1:]:
        moves = [
            ((g ^ flip) * shards + (s + step * near) % shards, g * shards + s)
            for g in range(groups)
            for s in range(shards)
        ]
        pieces.append(lax.ppermute(plane, AXES, moves))
    attended = finish(pieces, offsets, groups, shards, batch, q_heads // groups)
    return (got.reshape(1, groups, shards, block_len, width), attended)


def solution(mesh):
    return jax.shard_map(
        body,
        mesh=mesh,
        in_specs=(P("grp", "seq", None, None), P(), P(), P(), P(), P()),
        out_specs=(P(AXES, None, None, None, None), P()),
        check_vma=False,
    )
```

```python
import functools
import math

import jax
import jax.numpy as jnp
from jax import lax
from jax.experimental import pallas as pl
from jax.experimental.pallas import tpu as pltpu
from jax.sharding import PartitionSpec as P


AXES = ("grp", "seq")
F32 = jnp.float32
BF16 = jnp.bfloat16
NEAR_BYTES = 1 << 20
NEAR_DEVICES = 4


def three_parts(x):
    parts = []
    for _ in range(3):
        part = x.astype(BF16)
        parts.append(part)
        x = x - part.astype(F32)
    return jnp.concatenate(parts, axis=0)


def exact_dot(x, y, contract):
    rows = x.shape[0]
    wide = lax.dot_general(
        three_parts(x),
        y,
        (contract, ((), ())),
        preferred_element_type=F32,
    )
    return wide[:rows] + (wide[rows : 2 * rows] + wide[2 * rows :])


def in_vmem(shape):
    return 4 * math.prod(shape) <= NEAR_BYTES


def start_kernel(
    per_seq,
    dest_hbm,
    length_hbm,
    lat_hbm,
    key_hbm,
    value_hbm,
    query_hbm,
    out_hbm,
    mine_ref,
    dest,
    length,
    lat_ref,
    key_ref,
    value_ref,
    query_ref,
    ordered_ref,
    sems,
):
    slots, block_len, width = lat_ref.shape
    rank = width // 2
    heads, head_dim = query_ref.shape
    per_group = key_ref.shape[1] // head_dim
    per_kv = heads // per_group
    scale = 1.0 / float(head_dim) ** 0.5
    group = lax.axis_index("grp")
    first = lax.axis_index("seq") * slots
    seq = first // per_seq
    start = (first % per_seq) * block_len
    rows = pl.ds(pl.multiple_of(group * heads, heads), heads)
    sources = (lat_hbm, dest_hbm, key_hbm.at[group], query_hbm.at[seq, rows], length_hbm, value_hbm.at[group])
    targets = (lat_ref, dest, key_ref, query_ref, length, value_ref)
    copies = [
        pltpu.make_async_copy(source, target, sems.at[k])
        for k, (source, target) in enumerate(zip(sources, targets))
    ]
    for copy in copies:
        copy.start()
    for copy in copies:
        copy.wait()

    def move(j, carry):
        ordered_ref[dest[first + j]] = lat_ref[j]
        return carry

    lax.fori_loop(0, slots, move, 0, unroll=8)
    send = pltpu.make_async_copy(ordered_ref, out_hbm, sems.at[len(copies)])
    send.start()

    tokens = slots * block_len
    lat = lat_ref[...].reshape(tokens, width)
    absorbed = []
    for k in range(per_group):
        columns = slice(k * head_dim, (k + 1) * head_dim)
        absorbed.append(
            lax.dot_general(
                query_ref[k * per_kv : (k + 1) * per_kv, :],
                key_ref[:, columns],
                (((1,), (1,)), ((), ())),
                preferred_element_type=F32,
            )
        )
    absorbed = jnp.concatenate(absorbed, axis=0)
    scores = exact_dot(absorbed, lat[:, :rank], ((1,), (1,))) * scale
    position = start + lax.broadcasted_iota(jnp.int32, scores.shape, 1)
    live = position < length[seq]
    scores = jnp.where(live, scores, -1e30)
    top = jnp.max(scores, axis=1, keepdims=True)
    weights = jnp.where(live, jnp.exp(scores - top), 0.0)
    total = jnp.sum(weights, axis=1, keepdims=True)
    mixed = exact_dot(weights, lat[:, rank:], ((1,), (0,)))
    if per_seq == slots:
        mixed = mixed / total
    attended = []
    for k in range(per_group):
        columns = slice(k * head_dim, (k + 1) * head_dim)
        attended.append(
            exact_dot(mixed[k * per_kv : (k + 1) * per_kv], value_ref[:, columns], ((1,), (0,)))
        )
    fields = [jnp.concatenate(attended, axis=0)]
    if per_seq != slots:
        fields += [jnp.broadcast_to(field, (heads, head_dim)) for field in (top, total)]
    mine_ref[...] = jnp.concatenate(fields, axis=0)
    send.wait()


def start(latent, up_key, up_value, queries, lengths, block_dest):
    batch, q_heads, head_dim = queries.shape
    heads = q_heads // up_key.shape[0]
    per_seq = block_dest.shape[0] // batch
    rows = heads if per_seq == latent.shape[0] else 3 * heads
    return pl.pallas_call(
        functools.partial(start_kernel, per_seq),
        out_shape=(
            jax.ShapeDtypeStruct(latent.shape, latent.dtype),
            pltpu.VMEM((rows, head_dim), F32),
        ),
        in_specs=[pl.BlockSpec(memory_space=pl.ANY)] * 6,
        out_specs=(pl.BlockSpec(memory_space=pl.ANY), pl.BlockSpec(memory_space=pltpu.VMEM)),
        scratch_shapes=[
            pltpu.SMEM(block_dest.shape, jnp.int32),
            pltpu.SMEM(lengths.shape, jnp.int32),
            pltpu.VMEM(latent.shape, latent.dtype),
            pltpu.VMEM(up_key.shape[1:], up_key.dtype),
            pltpu.VMEM(up_value.shape[1:], up_value.dtype),
            pltpu.VMEM((heads, head_dim), queries.dtype),
            pltpu.VMEM(latent.shape, latent.dtype),
            pltpu.SemaphoreType.DMA((7,)),
        ],
        name="start",
    )(block_dest, lengths, latent, up_key, up_value, queries)


def finish_kernel(groups, shards, offsets, heads, got_ref, every_ref, blocks_hbm, result_hbm, result_ref, wide_ref, sems):
    copy_blocks = pltpu.make_async_copy(got_ref, blocks_hbm, sems.at[0])
    copy_blocks.start()
    batch = result_ref.shape[0]
    spans = shards // batch
    near, halves = every_ref.shape[0], every_ref.shape[2]
    group = lax.axis_index("grp")
    major = lax.axis_index("seq") // near
    for p, (step, flip) in enumerate(offsets):
        from_major = (major + step) % (shards // near)
        for half in range(halves):
            from_group = group ^ flip ^ (half * (groups // 2))
            for k in range(near):
                wide_ref[from_group, from_major * near + k] = every_ref[k, p, half]
    if spans > 1:
        for g in range(groups):
            for b in range(batch):
                parts = [wide_ref[g, b * spans + k] for k in range(spans)]
                accums, tops, totals = (
                    [part[f * heads : (f + 1) * heads] for part in parts] for f in range(3)
                )
                top = functools.reduce(jnp.maximum, tops)
                factors = [jnp.exp(t - top) for t in tops]
                accum = sum(x * f for x, f in zip(accums, factors))
                total = sum(x * f for x, f in zip(totals, factors))
                wide_ref[g, b, :heads] = accum / total
    head_dim = every_ref.shape[4]
    for g in range(groups):
        for h in range(heads):
            column = (g * heads + h) * head_dim
            result_ref[:, column : column + head_dim] = wide_ref[g, :batch, h, :]
    copy_result = pltpu.make_async_copy(result_ref, result_hbm, sems.at[1])
    copy_result.start()
    copy_blocks.wait()
    copy_result.wait()


def finish(got, every, offsets, groups, shards, batch, heads):
    rows, head_dim = every.shape[3:]
    columns = groups * heads * head_dim
    if in_vmem(every.shape) and in_vmem(got.shape):
        got = pltpu.with_memory_space_constraint(got, pltpu.VMEM)
        every = pltpu.with_memory_space_constraint(every, pltpu.VMEM)
    return pl.pallas_call(
        functools.partial(finish_kernel, groups, shards, offsets, heads),
        out_shape=(
            jax.ShapeDtypeStruct(got.shape, got.dtype),
            jax.ShapeDtypeStruct((batch, columns), F32),
        ),
        in_specs=[pl.BlockSpec(memory_space=pltpu.VMEM)] * 2,
        out_specs=(pl.BlockSpec(memory_space=pl.ANY),) * 2,
        scratch_shapes=[
            pltpu.VMEM((batch, columns), F32),
            pltpu.VMEM((groups, shards, rows, head_dim), F32),
            pltpu.SemaphoreType.DMA((2,)),
        ],
        name="finish",
    )(got, every)


def body(latent, up_key, up_value, queries, lengths, block_dest):
    groups = up_key.shape[0]
    _, block_len, width = latent.shape[1:]
    batch, q_heads, _ = queries.shape
    shards = lax.axis_size("seq")
    near = math.gcd(shards, NEAR_DEVICES)
    far = shards // near
    assert groups % 2 == 0 and shards % batch == 0
    payload, mine = start(latent[0], up_key, up_value, queries, lengths, block_dest)
    other = lax.ppermute(mine, "grp", [(i, i ^ (groups // 2)) for i in range(groups)])
    got = lax.all_to_all(payload, AXES, split_axis=0, concat_axis=0, tiled=True)
    both = jnp.stack([mine, other])
    offsets = [(step, flip) for flip in range(groups // 2) for step in range(far)]
    pieces = [both]
    for step, flip in offsets[1:]:
        moves = [
            ((g ^ flip) * shards + (s + step * near) % shards, g * shards + s)
            for g in range(groups)
            for s in range(shards)
        ]
        pieces.append(lax.ppermute(both, AXES, moves))
    neighbours = [[k * near + i for i in range(near)] for k in range(far)]
    every = lax.all_gather(jnp.stack(pieces), "seq", axis=0, axis_index_groups=neighbours)
    blocks, attended = finish(got, every, offsets, groups, shards, batch, q_heads // groups)
    return (blocks.reshape(1, groups, shards, block_len, width), attended)


def solution(mesh):
    return jax.shard_map(
        body,
        mesh=mesh,
        in_specs=(P("grp", "seq", None, None), P(), P(), P(), P(), P()),
        out_specs=(P(AXES, None, None, None, None), P()),
        check_vma=False,
    )
```

```python
import functools
import math

import jax
import jax.numpy as jnp
from jax import lax
from jax.experimental import pallas as pl
from jax.experimental.pallas import tpu as pltpu
from jax.sharding import PartitionSpec as P


AXES = ("grp", "seq")
F32 = jnp.float32
BF16 = jnp.bfloat16
NEAR_BYTES = 1 << 20
NEAR_DEVICES = 4


def three_parts(x):
    parts = []
    for _ in range(3):
        part = x.astype(BF16)
        parts.append(part)
        x = x - part.astype(F32)
    return jnp.concatenate(parts, axis=0)


def exact_dot(x, y, contract):
    rows = x.shape[0]
    wide = lax.dot_general(
        three_parts(x),
        y,
        (contract, ((), ())),
        preferred_element_type=F32,
    )
    return wide[:rows] + (wide[rows : 2 * rows] + wide[2 * rows :])


def in_vmem(shape):
    return 4 * math.prod(shape) <= NEAR_BYTES


def start_kernel(
    per_seq,
    dest_hbm,
    length_hbm,
    lat_hbm,
    key_hbm,
    value_hbm,
    query_hbm,
    out_hbm,
    mine_ref,
    dest,
    length,
    lat_ref,
    key_ref,
    value_ref,
    query_ref,
    ordered_ref,
    sems,
):
    slots, block_len, width = lat_ref.shape
    rank = width // 2
    heads, head_dim = query_ref.shape
    per_group = key_ref.shape[1] // head_dim
    per_kv = heads // per_group
    scale = 1.0 / float(head_dim) ** 0.5
    group = lax.axis_index("grp")
    first = lax.axis_index("seq") * slots
    seq = first // per_seq
    start = (first % per_seq) * block_len
    rows = pl.ds(pl.multiple_of(group * heads, heads), heads)
    sources = (lat_hbm, dest_hbm, key_hbm.at[group], query_hbm.at[seq, rows], length_hbm, value_hbm.at[group])
    targets = (lat_ref, dest, key_ref, query_ref, length, value_ref)
    copies = [
        pltpu.make_async_copy(source, target, sems.at[k])
        for k, (source, target) in enumerate(zip(sources, targets))
    ]
    for copy in copies:
        copy.start()
    for copy in copies:
        copy.wait()

    def move(j, carry):
        ordered_ref[dest[first + j]] = lat_ref[j]
        return carry

    lax.fori_loop(0, slots, move, 0, unroll=8)
    send = pltpu.make_async_copy(ordered_ref, out_hbm, sems.at[len(copies)])
    send.start()

    tokens = slots * block_len
    lat = lat_ref[...].reshape(tokens, width)
    absorbed = []
    for k in range(per_group):
        columns = slice(k * head_dim, (k + 1) * head_dim)
        absorbed.append(
            lax.dot_general(
                query_ref[k * per_kv : (k + 1) * per_kv, :],
                key_ref[:, columns],
                (((1,), (1,)), ((), ())),
                preferred_element_type=F32,
            )
        )
    absorbed = jnp.concatenate(absorbed, axis=0)
    scores = exact_dot(absorbed, lat[:, :rank], ((1,), (1,))) * scale
    position = start + lax.broadcasted_iota(jnp.int32, scores.shape, 1)
    live = position < length[seq]
    scores = jnp.where(live, scores, -1e30)
    top = jnp.max(scores, axis=1, keepdims=True)
    weights = jnp.where(live, jnp.exp(scores - top), 0.0)
    total = jnp.sum(weights, axis=1, keepdims=True)
    mixed = exact_dot(weights, lat[:, rank:], ((1,), (0,)))
    if per_seq == slots:
        mixed = mixed / total
    attended = []
    for k in range(per_group):
        columns = slice(k * head_dim, (k + 1) * head_dim)
        attended.append(
            exact_dot(mixed[k * per_kv : (k + 1) * per_kv], value_ref[:, columns], ((1,), (0,)))
        )
    fields = [jnp.concatenate(attended, axis=0)]
    if per_seq != slots:
        fields += [jnp.broadcast_to(field, (heads, head_dim)) for field in (top, total)]
    mine_ref[...] = jnp.concatenate(fields, axis=0)
    send.wait()


def start(latent, up_key, up_value, queries, lengths, block_dest):
    batch, q_heads, head_dim = queries.shape
    heads = q_heads // up_key.shape[0]
    per_seq = block_dest.shape[0] // batch
    rows = heads if per_seq == latent.shape[0] else 3 * heads
    return pl.pallas_call(
        functools.partial(start_kernel, per_seq),
        out_shape=(
            jax.ShapeDtypeStruct(latent.shape, latent.dtype),
            pltpu.VMEM((rows, head_dim), F32),
        ),
        in_specs=[pl.BlockSpec(memory_space=pl.ANY)] * 6,
        out_specs=(pl.BlockSpec(memory_space=pl.ANY), pl.BlockSpec(memory_space=pltpu.VMEM)),
        scratch_shapes=[
            pltpu.SMEM(block_dest.shape, jnp.int32),
            pltpu.SMEM(lengths.shape, jnp.int32),
            pltpu.VMEM(latent.shape, latent.dtype),
            pltpu.VMEM(up_key.shape[1:], up_key.dtype),
            pltpu.VMEM(up_value.shape[1:], up_value.dtype),
            pltpu.VMEM((heads, head_dim), queries.dtype),
            pltpu.VMEM(latent.shape, latent.dtype),
            pltpu.SemaphoreType.DMA((7,)),
        ],
        name="start",
    )(block_dest, lengths, latent, up_key, up_value, queries)


def finish_kernel(groups, shards, offsets, heads, got_ref, *refs):
    pieces, (blocks_hbm, result_hbm, result_ref, wide_ref, sems) = (
        refs[: len(offsets)],
        refs[len(offsets) :],
    )
    copy_blocks = pltpu.make_async_copy(got_ref, blocks_hbm, sems.at[0])
    copy_blocks.start()
    batch = result_ref.shape[0]
    spans = shards // batch
    near, halves, _, head_dim = pieces[0].shape
    group = lax.axis_index("grp")
    major = lax.axis_index("seq") // near
    for (step, flip), piece in zip(offsets, pieces):
        from_major = (major + step) % (shards // near)
        for half in range(halves):
            from_group = group ^ flip ^ (half * (groups // 2))
            for k in range(near):
                wide_ref[from_group, from_major * near + k] = piece[k, half]
    if spans > 1:
        for g in range(groups):
            for b in range(batch):
                parts = [wide_ref[g, b * spans + k] for k in range(spans)]
                accums, tops, totals = (
                    [part[f * heads : (f + 1) * heads] for part in parts] for f in range(3)
                )
                top = functools.reduce(jnp.maximum, tops)
                factors = [jnp.exp(t - top) for t in tops]
                accum = sum(x * f for x, f in zip(accums, factors))
                total = sum(x * f for x, f in zip(totals, factors))
                wide_ref[g, b, :heads] = accum / total
    for g in range(groups):
        for h in range(heads):
            column = (g * heads + h) * head_dim
            result_ref[:, column : column + head_dim] = wide_ref[g, :batch, h, :]
    copy_result = pltpu.make_async_copy(result_ref, result_hbm, sems.at[1])
    copy_result.start()
    copy_blocks.wait()
    copy_result.wait()


def finish(got, pieces, offsets, groups, shards, batch, heads):
    rows, head_dim = pieces[0].shape[2:]
    columns = groups * heads * head_dim
    if in_vmem(got.shape):
        got = pltpu.with_memory_space_constraint(got, pltpu.VMEM)
        pieces = [pltpu.with_memory_space_constraint(piece, pltpu.VMEM) for piece in pieces]
    return pl.pallas_call(
        functools.partial(finish_kernel, groups, shards, offsets, heads),
        out_shape=(
            jax.ShapeDtypeStruct(got.shape, got.dtype),
            jax.ShapeDtypeStruct((batch, columns), F32),
        ),
        in_specs=[pl.BlockSpec(memory_space=pltpu.VMEM)] * (1 + len(pieces)),
        out_specs=(pl.BlockSpec(memory_space=pl.ANY),) * 2,
        scratch_shapes=[
            pltpu.VMEM((batch, columns), F32),
            pltpu.VMEM((groups, shards, rows, head_dim), F32),
            pltpu.SemaphoreType.DMA((2,)),
        ],
        name="finish",
    )(got, *pieces)


def body(latent, up_key, up_value, queries, lengths, block_dest):
    groups = up_key.shape[0]
    _, block_len, width = latent.shape[1:]
    batch, q_heads, _ = queries.shape
    shards = lax.axis_size("seq")
    near = math.gcd(shards, NEAR_DEVICES)
    far = shards // near
    assert groups % 2 == 0 and shards % batch == 0
    payload, mine = start(latent[0], up_key, up_value, queries, lengths, block_dest)
    other = lax.ppermute(mine, "grp", [(i, i ^ (groups // 2)) for i in range(groups)])
    got = lax.all_to_all(payload, AXES, split_axis=0, concat_axis=0, tiled=True)
    both = jnp.stack([mine, other])
    neighbours = [[k * near + i for i in range(near)] for k in range(far)]
    plane = lax.all_gather(both, "seq", axis=0, axis_index_groups=neighbours)
    offsets = [(step, flip) for flip in range(groups // 2) for step in range(far)]
    pieces = [plane]
    for step, flip in offsets[1:]:
        moves = [
            ((g ^ flip) * shards + (s + step * near) % shards, g * shards + s)
            for g in range(groups)
            for s in range(shards)
        ]
        pieces.append(lax.ppermute(plane, AXES, moves))
    blocks, attended = finish(got, pieces, offsets, groups, shards, batch, q_heads // groups)
    return (blocks.reshape(1, groups, shards, block_len, width), attended)


def solution(mesh):
    return jax.shard_map(
        body,
        mesh=mesh,
        in_specs=(P("grp", "seq", None, None), P(), P(), P(), P(), P()),
        out_specs=(P(AXES, None, None, None, None), P()),
        check_vma=False,
    )
```

```python
import functools
import math

import jax
import jax.numpy as jnp
from jax import lax
from jax.experimental import pallas as pl
from jax.experimental.pallas import tpu as pltpu
from jax.sharding import PartitionSpec as P


AXES = ("grp", "seq")
F32 = jnp.float32
BF16 = jnp.bfloat16
NEAR_BYTES = 1 << 20
TAIL = 8
LANES = 128


def parts_of(x, count):
    parts = []
    for _ in range(count):
        part = x.astype(BF16)
        parts.append(part)
        x = x - part.astype(F32)
    return parts


def exact_dot(x, y, contract):
    rows = x.shape[0]
    wide = lax.dot_general(
        jnp.concatenate(parts_of(x, 3), axis=0),
        y,
        (contract, ((), ())),
        preferred_element_type=F32,
    )
    return wide[:rows] + (wide[rows : 2 * rows] + wide[2 * rows :])


def in_vmem(*arrays):
    if sum(math.prod(x.shape) * x.dtype.itemsize for x in arrays) > NEAR_BYTES:
        return arrays
    return tuple(pltpu.with_memory_space_constraint(x, pltpu.VMEM) for x in arrays)


def start_kernel(
    per_seq,
    sent,
    groups,
    shards,
    dest_hbm,
    length_hbm,
    lat_hbm,
    key_hbm,
    value_hbm,
    query_hbm,
    out_hbm,
    side_0,
    side_1,
    dest,
    length,
    lat_ref,
    key_ref,
    value_ref,
    query_ref,
    ordered_ref,
    tails_ref,
    sems,
):
    slots, block_len, width = lat_ref.shape
    kept = ordered_ref.shape[1]
    rank = width // 2
    heads, head_dim = query_ref.shape
    per_group = key_ref.shape[1] // head_dim
    per_kv = heads // per_group
    scale = 1.0 / float(head_dim) ** 0.5
    group = lax.axis_index("grp")
    shard = lax.axis_index("seq")
    first = shard * slots
    seq = first // per_seq
    begin = (first % per_seq) * block_len
    rows = pl.ds(pl.multiple_of(group * heads, heads), heads)
    sources = (lat_hbm, dest_hbm, key_hbm.at[group], query_hbm.at[seq, rows], length_hbm, value_hbm.at[group])
    targets = (lat_ref, dest, key_ref, query_ref, length, value_ref)
    copies = [
        pltpu.make_async_copy(source, target, sems.at[k])
        for k, (source, target) in enumerate(zip(sources, targets))
    ]
    for copy in copies:
        copy.start()
    for copy in copies:
        copy.wait()

    def move(j, carry):
        target = dest[first + j]
        for c in range(width // LANES):
            lanes = slice(c * LANES, (c + 1) * LANES)
            height = min(block_len, kept - c * block_len)
            ordered_ref[target, c * block_len : c * block_len + height, :] = lat_ref[j, :height, lanes]
        tails_ref[target] = lat_ref[j, block_len - TAIL :, width - LANES :]
        return carry

    lax.fori_loop(0, slots, move, 0, unroll=8)
    send = pltpu.make_async_copy(ordered_ref, out_hbm, sems.at[len(copies)])
    send.start()

    far = shards // 2
    half = groups // 2
    count = half * far
    sides = (side_0, side_1)
    for over in range(2):
        for core in range(2):
            for flip in range(half):
                for step in range(far):
                    target = ((group ^ flip) ^ (over * half)) * shards + (
                        (shard // 2 + step) % far * 2 + core
                    )
                    sides[over][core * count + flip * far + step] = tails_ref[target]

    tokens = slots * block_len
    lat = lat_ref[...].reshape(tokens, width)
    absorbed = []
    for k in range(per_group):
        columns = slice(k * head_dim, (k + 1) * head_dim)
        absorbed.append(
            lax.dot_general(
                query_ref[k * per_kv : (k + 1) * per_kv, :],
                key_ref[:, columns],
                (((1,), (1,)), ((), ())),
                preferred_element_type=F32,
            )
        )
    absorbed = jnp.concatenate(absorbed, axis=0)
    scores = exact_dot(absorbed, lat[:, :rank], ((1,), (1,))) * scale
    position = begin + lax.broadcasted_iota(jnp.int32, scores.shape, 1)
    live = position < length[seq]
    scores = jnp.where(live, scores, -1e30)
    top = jnp.max(scores, axis=1, keepdims=True)
    weights = jnp.where(live, jnp.exp(scores - top), 0.0)
    total = jnp.sum(weights, axis=1, keepdims=True)
    mixed = exact_dot(weights, lat[:, rank:], ((1,), (0,)))
    if per_seq == slots:
        mixed = mixed / total
    attended = []
    for k in range(per_group):
        columns = slice(k * head_dim, (k + 1) * head_dim)
        attended.append(
            exact_dot(mixed[k * per_kv : (k + 1) * per_kv], value_ref[:, columns], ((1,), (0,)))
        )
    fields = list(attended)
    if per_seq != slots:
        for field in (top, total):
            for k in range(per_group):
                fields.append(
                    jnp.broadcast_to(field[k * per_kv : (k + 1) * per_kv], (per_kv, head_dim))
                )
    parts = [part for field in fields for part in parts_of(field, sent)]
    for side in sides:
        for p, part in enumerate(parts):
            side[2 * count + p] = part
    send.wait()


def start(latent, up_key, up_value, queries, lengths, block_dest, groups, shards, sent, fields):
    _, block_len, width = latent.shape
    batch, q_heads, head_dim = queries.shape
    heads = q_heads // groups
    per_seq = block_dest.shape[0] // batch
    kept = block_len * (width // LANES) - TAIL
    dests = groups * shards
    side = (groups // 2 * shards + sent * fields, TAIL, LANES)
    vmem = pl.BlockSpec(memory_space=pltpu.VMEM)
    return pl.pallas_call(
        functools.partial(start_kernel, per_seq, sent, groups, shards),
        out_shape=(jax.ShapeDtypeStruct((dests, kept, LANES), latent.dtype),)
        + (pltpu.VMEM(side, latent.dtype),) * 2,
        in_specs=[pl.BlockSpec(memory_space=pl.ANY)] * 6,
        out_specs=(pl.BlockSpec(memory_space=pl.ANY),) + (vmem,) * 2,
        scratch_shapes=[
            pltpu.SMEM(block_dest.shape, jnp.int32),
            pltpu.SMEM(lengths.shape, jnp.int32),
            pltpu.VMEM(latent.shape, latent.dtype),
            pltpu.VMEM(up_key.shape[1:], up_key.dtype),
            pltpu.VMEM(up_value.shape[1:], up_value.dtype),
            pltpu.VMEM((heads, head_dim), queries.dtype),
            pltpu.VMEM((dests, kept, LANES), latent.dtype),
            pltpu.VMEM((dests, TAIL, LANES), latent.dtype),
            pltpu.SemaphoreType.DMA((7,)),
        ],
        name="start",
    )(block_dest, lengths, latent, up_key, up_value, queries)


def pack_kernel(pair_ref, *parcels):
    count = len(parcels)
    tiles = pair_ref.shape[2]
    core = lax.axis_index("seq") % 2
    for k, parcel in enumerate(parcels):
        for over in range(2):
            for source in range(2):
                q = over * 2 + source
                parcel[q, 0] = pair_ref[source, over, core * count + k]
                for p in range(tiles - 2 * count):
                    parcel[q, 1 + p] = pair_ref[source, over, 2 * count + p]


def pack(pair, count):
    tiles, tail, width = pair.shape[2:]
    parcel = (4, 1 + tiles - 2 * count, tail, width)
    (pair,) = in_vmem(pair)
    vmem = pl.BlockSpec(memory_space=pltpu.VMEM)
    small = 2 * count * math.prod(parcel) <= NEAR_BYTES
    shape = (pltpu.VMEM if small else jax.ShapeDtypeStruct)(parcel, pair.dtype)
    return pl.pallas_call(
        pack_kernel,
        out_shape=(shape,) * count,
        in_specs=[vmem],
        out_specs=(vmem,) * count,
        name="pack",
    )(pair)


def finish_kernel(groups, shards, offsets, sent, got_ref, *refs):
    count = len(offsets)
    parcels, (blocks_hbm, result_hbm, result_ref, wide_ref, tails_ref, sems) = refs[:count], refs[count:]
    kept = got_ref.shape[1]
    block_len, width = blocks_hbm.shape[1:]
    copies = []
    for c in range(width // LANES):
        height = min(block_len, kept - c * block_len)
        copies.append(
            pltpu.make_async_copy(
                got_ref.at[:, pl.ds(c * block_len, height), :],
                blocks_hbm.at[:, pl.ds(0, height), pl.ds(c * LANES, LANES)],
                sems.at[c],
            )
        )
        copies[-1].start()
    batch, _ = result_ref.shape
    spans = shards // batch
    far, half = shards // 2, groups // 2
    fields, per_group = wide_ref.shape[2:4]
    group = lax.axis_index("grp")
    shard = lax.axis_index("seq")
    for (flip, step), parcel in zip(offsets, parcels):
        for q in range(4):
            source_group = (group ^ flip) ^ (q // 2 * half)
            source_shard = (shard // 2 - step + far) % far * 2 + q % 2
            tails_ref[source_group * shards + source_shard] = parcel[q, 0]
            for f in range(fields):
                for k in range(per_group):
                    first = 1 + (f * per_group + k) * sent
                    wide_ref[source_group, source_shard, f, k] = sum(
                        parcel[q, first + p].astype(F32) for p in reversed(range(sent))
                    )
    copies.append(
        pltpu.make_async_copy(
            tails_ref,
            blocks_hbm.at[:, pl.ds(block_len - TAIL, TAIL), pl.ds(width - LANES, LANES)],
            sems.at[width // LANES],
        )
    )
    copies[-1].start()
    if spans > 1:
        for g in range(groups):
            for b in range(batch):
                pieces = [wide_ref[g, b * spans + k] for k in range(spans)]
                top = functools.reduce(jnp.maximum, [piece[1] for piece in pieces])
                factors = [jnp.exp(piece[1] - top) for piece in pieces]
                accum = sum(piece[0] * f for piece, f in zip(pieces, factors))
                total = sum(piece[2] * f for piece, f in zip(pieces, factors))
                wide_ref[g, b, 0] = accum / total
    for g in range(groups):
        for k in range(per_group):
            for j in range(TAIL):
                column = ((g * per_group + k) * TAIL + j) * LANES
                result_ref[:, column : column + LANES] = wide_ref[g, :batch, 0, k, j, :]
    copies.append(pltpu.make_async_copy(result_ref, result_hbm, sems.at[width // LANES + 1]))
    copies[-1].start()
    for copy in copies:
        copy.wait()


def finish(got, parcels, offsets, groups, shards, batch, block_len, width, per_group, sent):
    dests = got.shape[0]
    fields = (parcels[0].shape[1] - 1) // (sent * per_group)
    columns = groups * per_group * TAIL * LANES
    got, *parcels = in_vmem(got, *parcels)
    return pl.pallas_call(
        functools.partial(finish_kernel, groups, shards, offsets, sent),
        out_shape=(
            jax.ShapeDtypeStruct((dests, block_len, width), got.dtype),
            jax.ShapeDtypeStruct((batch, columns), F32),
        ),
        in_specs=[pl.BlockSpec(memory_space=pltpu.VMEM)] * (1 + len(parcels)),
        out_specs=(pl.BlockSpec(memory_space=pl.ANY),) * 2,
        scratch_shapes=[
            pltpu.VMEM((batch, columns), F32),
            pltpu.VMEM((groups, shards, fields, per_group, TAIL, LANES), F32),
            pltpu.VMEM((dests, TAIL, LANES), got.dtype),
            pltpu.SemaphoreType.DMA((width // LANES + 2,)),
        ],
        name="finish",
    )(got, *parcels)


def sending_order(half, far):
    even, odd = list(range(0, far, 2)), list(range(1, far, 2))
    order = [(flip, step) for flip in range(half - 1, 0, -1) for step in odd + even[::-1]]
    return order + [(0, step) for step in even[1:] + odd]


def body(latent, up_key, up_value, queries, lengths, block_dest):
    groups = up_key.shape[0]
    _, block_len, width = latent.shape[1:]
    batch, q_heads, head_dim = queries.shape
    shards = lax.axis_size("seq")
    far, half = shards // 2, groups // 2
    assert groups == 2 * half and shards == 2 * far and shards % batch == 0
    per_group = up_key.shape[2] // head_dim
    assert head_dim == LANES and q_heads == groups * per_group * TAIL
    sent, fields = (2, 1) if shards == batch else (3, 3)
    payload, mine, other = start(
        latent[0], up_key, up_value, queries, lengths, block_dest, groups, shards, sent, fields * per_group
    )
    devices = [(g, s) for g in range(groups) for s in range(shards)]
    other = lax.ppermute(other, "grp", [(g, g ^ half) for g in range(groups)])
    got = lax.all_to_all(payload, AXES, split_axis=0, concat_axis=0, tiled=True)
    cores = [[2 * k, 2 * k + 1] for k in range(far)]
    pair = lax.all_gather(jnp.stack([mine, other]), "seq", axis=0, axis_index_groups=cores)
    offsets = [(flip, step) for flip in range(half) for step in range(far)]
    parcels = list(pack(pair, len(offsets)))
    for flip, step in sending_order(half, far):
        k = offsets.index((flip, step))
        moves = [(g * shards + s, (g ^ flip) * shards + (s + 2 * step) % shards) for g, s in devices]
        parcels[k] = lax.ppermute(parcels[k], AXES, moves)
    blocks, attended = finish(
        got, parcels, offsets, groups, shards, batch, block_len, width, per_group, sent
    )
    return (blocks.reshape(1, groups, shards, block_len, width), attended)


def solution(mesh):
    return jax.shard_map(
        body,
        mesh=mesh,
        in_specs=(P("grp", "seq", None, None), P(), P(), P(), P(), P()),
        out_specs=(P(AXES, None, None, None, None), P()),
        check_vma=False,
    )
```

```python
import functools
import math

import jax
import jax.numpy as jnp
from jax import lax
from jax.experimental import pallas as pl
from jax.experimental.pallas import tpu as pltpu
from jax.sharding import PartitionSpec as P


AXES = ("grp", "seq")
F32 = jnp.float32
BF16 = jnp.bfloat16
NEAR_BYTES = 1 << 20
TAIL = 8
LANES = 128


def parts_of(x, count):
    parts = []
    for _ in range(count):
        part = x.astype(BF16)
        parts.append(part)
        x = x - part.astype(F32)
    return parts


def exact_dot(x, y, contract):
    rows = x.shape[0]
    wide = lax.dot_general(
        jnp.concatenate(parts_of(x, 3), axis=0),
        y,
        (contract, ((), ())),
        preferred_element_type=F32,
    )
    return wide[:rows] + (wide[rows : 2 * rows] + wide[2 * rows :])


def in_vmem(*arrays):
    if sum(math.prod(x.shape) * x.dtype.itemsize for x in arrays) > NEAR_BYTES:
        return arrays
    return tuple(pltpu.with_memory_space_constraint(x, pltpu.VMEM) for x in arrays)


def start_kernel(
    per_seq,
    sent,
    groups,
    shards,
    dest_hbm,
    length_hbm,
    lat_hbm,
    key_hbm,
    value_hbm,
    query_hbm,
    out_hbm,
    side_0,
    side_1,
    dest,
    length,
    lat_ref,
    key_ref,
    value_ref,
    query_ref,
    ordered_ref,
    tails_ref,
    sems,
):
    slots, block_len, width = lat_ref.shape
    kept = ordered_ref.shape[1]
    rank = width // 2
    heads, head_dim = query_ref.shape
    per_group = key_ref.shape[1] // head_dim
    per_kv = heads // per_group
    scale = 1.0 / float(head_dim) ** 0.5
    group = lax.axis_index("grp")
    shard = lax.axis_index("seq")
    first = shard * slots
    seq = first // per_seq
    begin = (first % per_seq) * block_len
    rows = pl.ds(pl.multiple_of(group * heads, heads), heads)
    sources = (lat_hbm, dest_hbm, key_hbm.at[group], query_hbm.at[seq, rows], length_hbm, value_hbm.at[group])
    targets = (lat_ref, dest, key_ref, query_ref, length, value_ref)
    copies = [
        pltpu.make_async_copy(source, target, sems.at[k])
        for k, (source, target) in enumerate(zip(sources, targets))
    ]
    for copy in copies:
        copy.start()
    for copy in copies:
        copy.wait()

    def move(j, carry):
        target = dest[first + j]
        for c in range(width // LANES):
            lanes = slice(c * LANES, (c + 1) * LANES)
            height = min(block_len, kept - c * block_len)
            ordered_ref[target, c * block_len : c * block_len + height, :] = lat_ref[j, :height, lanes]
        tails_ref[target] = lat_ref[j, block_len - TAIL :, width - LANES :]
        return carry

    lax.fori_loop(0, slots, move, 0, unroll=min(slots, 32))
    send = pltpu.make_async_copy(ordered_ref, out_hbm, sems.at[len(copies)])
    send.start()

    far = shards // 2
    half = groups // 2
    count = half * far
    sides = (side_0, side_1)
    for over in range(2):
        for core in range(2):
            for flip in range(half):
                for step in range(far):
                    target = ((group ^ flip) ^ (over * half)) * shards + (
                        (shard // 2 + step) % far * 2 + core
                    )
                    sides[over][core * count + flip * far + step] = tails_ref[target]

    tokens = slots * block_len
    lat = lat_ref[...].reshape(tokens, width)
    absorbed = []
    for k in range(per_group):
        columns = slice(k * head_dim, (k + 1) * head_dim)
        absorbed.append(
            lax.dot_general(
                query_ref[k * per_kv : (k + 1) * per_kv, :],
                key_ref[:, columns],
                (((1,), (1,)), ((), ())),
                preferred_element_type=F32,
            )
        )
    absorbed = jnp.concatenate(absorbed, axis=0)
    scores = exact_dot(absorbed, lat[:, :rank], ((1,), (1,))) * scale
    position = begin + lax.broadcasted_iota(jnp.int32, scores.shape, 1)
    live = position < length[seq]
    scores = jnp.where(live, scores, -1e30)
    top = jnp.max(scores, axis=1, keepdims=True)
    weights = jnp.where(live, jnp.exp(scores - top), 0.0)
    total = jnp.sum(weights, axis=1, keepdims=True)
    mixed = exact_dot(weights, lat[:, rank:], ((1,), (0,)))
    if per_seq == slots:
        mixed = mixed / total
    attended = []
    for k in range(per_group):
        columns = slice(k * head_dim, (k + 1) * head_dim)
        attended.append(
            exact_dot(mixed[k * per_kv : (k + 1) * per_kv], value_ref[:, columns], ((1,), (0,)))
        )
    fields = list(attended)
    if per_seq != slots:
        for field in (top, total):
            for k in range(per_group):
                fields.append(
                    jnp.broadcast_to(field[k * per_kv : (k + 1) * per_kv], (per_kv, head_dim))
                )
    parts = [part for field in fields for part in parts_of(field, sent)]
    for side in sides:
        for p, part in enumerate(parts):
            side[2 * count + p] = part
    send.wait()


def start(latent, up_key, up_value, queries, lengths, block_dest, groups, shards, sent, fields):
    _, block_len, width = latent.shape
    batch, q_heads, head_dim = queries.shape
    heads = q_heads // groups
    per_seq = block_dest.shape[0] // batch
    kept = block_len * (width // LANES) - TAIL
    dests = groups * shards
    side = (groups // 2 * shards + sent * fields, TAIL, LANES)
    vmem = pl.BlockSpec(memory_space=pltpu.VMEM)
    return pl.pallas_call(
        functools.partial(start_kernel, per_seq, sent, groups, shards),
        out_shape=(jax.ShapeDtypeStruct((dests, kept, LANES), latent.dtype),)
        + (pltpu.VMEM(side, latent.dtype),) * 2,
        in_specs=[pl.BlockSpec(memory_space=pl.ANY)] * 6,
        out_specs=(pl.BlockSpec(memory_space=pl.ANY),) + (vmem,) * 2,
        scratch_shapes=[
            pltpu.SMEM(block_dest.shape, jnp.int32),
            pltpu.SMEM(lengths.shape, jnp.int32),
            pltpu.VMEM(latent.shape, latent.dtype),
            pltpu.VMEM(up_key.shape[1:], up_key.dtype),
            pltpu.VMEM(up_value.shape[1:], up_value.dtype),
            pltpu.VMEM((heads, head_dim), queries.dtype),
            pltpu.VMEM((dests, kept, LANES), latent.dtype),
            pltpu.VMEM((dests, TAIL, LANES), latent.dtype),
            pltpu.SemaphoreType.DMA((7,)),
        ],
        name="start",
    )(block_dest, lengths, latent, up_key, up_value, queries)


def pack_kernel(mine_ref, other_ref, *parcels):
    count = len(parcels)
    tiles = mine_ref.shape[1]
    core = lax.axis_index("seq") % 2
    for k, parcel in enumerate(parcels):
        for over in range(2):
            for swap, pair_ref in enumerate((mine_ref, other_ref)):
                q = over * 2 + swap
                parcel[q, 0] = pair_ref[over, core * count + k]
                for p in range(tiles - 2 * count):
                    parcel[q, 1 + p] = pair_ref[over, 2 * count + p]


def pack(mine, other, count):
    tiles, tail, width = mine.shape[1:]
    parcel = (4, 1 + tiles - 2 * count, tail, width)
    mine, other = in_vmem(mine, other)
    vmem = pl.BlockSpec(memory_space=pltpu.VMEM)
    small = 2 * count * math.prod(parcel) <= NEAR_BYTES
    shape = (pltpu.VMEM if small else jax.ShapeDtypeStruct)(parcel, mine.dtype)
    return pl.pallas_call(
        pack_kernel,
        out_shape=(shape,) * count,
        in_specs=[vmem] * 2,
        out_specs=(vmem,) * count,
        name="pack",
    )(mine, other)


def finish_kernel(groups, shards, offsets, sent, got_ref, *refs):
    count = len(offsets)
    parcels, (blocks_hbm, result_hbm, result_ref, wide_ref, tails_ref, sems) = refs[:count], refs[count:]
    kept = got_ref.shape[1]
    block_len, width = blocks_hbm.shape[1:]
    copies = []
    for c in range(width // LANES):
        height = min(block_len, kept - c * block_len)
        copies.append(
            pltpu.make_async_copy(
                got_ref.at[:, pl.ds(c * block_len, height), :],
                blocks_hbm.at[:, pl.ds(0, height), pl.ds(c * LANES, LANES)],
                sems.at[c],
            )
        )
        copies[-1].start()
    batch, _ = result_ref.shape
    spans = shards // batch
    far, half = shards // 2, groups // 2
    fields, per_group = wide_ref.shape[2:4]
    group = lax.axis_index("grp")
    shard = lax.axis_index("seq")
    for (flip, step), parcel in zip(offsets, parcels):
        for q in range(4):
            source_group = (group ^ flip) ^ (q // 2 * half)
            source_shard = (shard // 2 - step + far) % far * 2 + (shard + q) % 2
            tails_ref[source_group * shards + source_shard] = parcel[q, 0]
            for f in range(fields):
                for k in range(per_group):
                    first = 1 + (f * per_group + k) * sent
                    wide_ref[source_group, source_shard, f, k] = sum(
                        parcel[q, first + p].astype(F32) for p in reversed(range(sent))
                    )
    copies.append(
        pltpu.make_async_copy(
            tails_ref,
            blocks_hbm.at[:, pl.ds(block_len - TAIL, TAIL), pl.ds(width - LANES, LANES)],
            sems.at[width // LANES],
        )
    )
    copies[-1].start()
    if spans > 1:
        for g in range(groups):
            for b in range(batch):
                pieces = [wide_ref[g, b * spans + k] for k in range(spans)]
                top = functools.reduce(jnp.maximum, [piece[1] for piece in pieces])
                factors = [jnp.exp(piece[1] - top) for piece in pieces]
                accum = sum(piece[0] * f for piece, f in zip(pieces, factors))
                total = sum(piece[2] * f for piece, f in zip(pieces, factors))
                wide_ref[g, b, 0] = accum / total
    for g in range(groups):
        for k in range(per_group):
            for j in range(TAIL):
                column = ((g * per_group + k) * TAIL + j) * LANES
                result_ref[:, column : column + LANES] = wide_ref[g, :batch, 0, k, j, :]
    copies.append(pltpu.make_async_copy(result_ref, result_hbm, sems.at[width // LANES + 1]))
    copies[-1].start()
    for copy in copies:
        copy.wait()


def finish(got, parcels, offsets, groups, shards, batch, block_len, width, per_group, sent):
    dests = got.shape[0]
    fields = (parcels[0].shape[1] - 1) // (sent * per_group)
    columns = groups * per_group * TAIL * LANES
    got, *parcels = in_vmem(got, *parcels)
    return pl.pallas_call(
        functools.partial(finish_kernel, groups, shards, offsets, sent),
        out_shape=(
            jax.ShapeDtypeStruct((dests, block_len, width), got.dtype),
            jax.ShapeDtypeStruct((batch, columns), F32),
        ),
        in_specs=[pl.BlockSpec(memory_space=pltpu.VMEM)] * (1 + len(parcels)),
        out_specs=(pl.BlockSpec(memory_space=pl.ANY),) * 2,
        scratch_shapes=[
            pltpu.VMEM((batch, columns), F32),
            pltpu.VMEM((groups, shards, fields, per_group, TAIL, LANES), F32),
            pltpu.VMEM((dests, TAIL, LANES), got.dtype),
            pltpu.SemaphoreType.DMA((width // LANES + 2,)),
        ],
        name="finish",
    )(got, *parcels)


def sending_order(half, far):
    steps = list(range(1, far, 2)) + list(range(0, far, 2))[::-1]
    across = [(flip, step) for flip in range(half - 1, 0, -1) for step in steps]
    within = [(0, step) for step in range(1, far)]
    order = []
    for n in range(0, max(len(across), len(within)), 2):
        order += across[n : n + 2] + within[n : n + 2]
    return order


def body(latent, up_key, up_value, queries, lengths, block_dest):
    groups = up_key.shape[0]
    _, block_len, width = latent.shape[1:]
    batch, q_heads, head_dim = queries.shape
    shards = lax.axis_size("seq")
    far, half = shards // 2, groups // 2
    assert groups == 2 * half and shards == 2 * far and shards % batch == 0
    per_group = up_key.shape[2] // head_dim
    assert head_dim == LANES and q_heads == groups * per_group * TAIL
    sent, fields = (2, 1) if shards == batch else (3, 3)
    payload, mine, other = start(
        latent[0], up_key, up_value, queries, lengths, block_dest, groups, shards, sent, fields * per_group
    )
    devices = [(g, s) for g in range(groups) for s in range(shards)]
    other = lax.ppermute(other, "grp", [(g, g ^ half) for g in range(groups)])
    got = lax.all_to_all(payload, AXES, split_axis=0, concat_axis=0, tiled=True)
    pair = jnp.stack([mine, other])
    beside = lax.ppermute(pair, "seq", [(s, s ^ 1) for s in range(shards)])
    offsets = [(flip, step) for flip in range(half) for step in range(far)]
    parcels = list(pack(pair, beside, len(offsets)))
    for flip, step in sending_order(half, far):
        k = offsets.index((flip, step))
        moves = [(g * shards + s, (g ^ flip) * shards + (s + 2 * step) % shards) for g, s in devices]
        parcels[k] = lax.ppermute(parcels[k], AXES, moves)
    blocks, attended = finish(
        got, parcels, offsets, groups, shards, batch, block_len, width, per_group, sent
    )
    return (blocks.reshape(1, groups, shards, block_len, width), attended)


def solution(mesh):
    return jax.shard_map(
        body,
        mesh=mesh,
        in_specs=(P("grp", "seq", None, None), P(), P(), P(), P(), P()),
        out_specs=(P(AXES, None, None, None, None), P()),
        check_vma=False,
    )
```
